128 devices in a mesh: node: 128 (over z, x, y, core).
Axes of the slice: x: 4, y: 4, z: 4, core: 2. Of those that a mesh axis runs over, the one named last changes fastest.
Arguments:
- labels: bfloat16 [524288, 512], P('node'), may hold values from -6 to 6
- seed_mask: int32 [524288], P('node'), may hold values 0 or 1
- band_w: bfloat16 [4096, 3, 128, 128], P('node'), may hold values from 0.0009994507 to 1
- far_block: int32 [128, 128, 2], P('node'), may hold values from 0 to 511
- far_tile: int32 [128, 128, 2], P('node'), may hold values from 0 to 31
- far_count: int32 [128, 128], P('node'), may hold values from 0 to 2, as said below
- far_w: bfloat16 [128, 128, 2, 8, 128], P('node'), may hold values from 0.049804688 to 2
Outputs:
- final_labels: bfloat16 [524288, 512], P('node')
- residual: float32 [2, 4096], P(None, 'node')
The draws below stay inside these ranges and needn't reach their ends.
Inputs may be any that keep to these rules, and one draw needn't show every extreme that they name: `far_count`: in every draw at least one destination shard has all 2 slots live from every source shard; other counts vary from pair to pair.
All inputs are finite; a program needn't handle non-finite values. No bound on the sum of `seed_mask` on one device may be relied on, other than what follows from the above.
Results may differ from the reference program's by a relative error of at most 0.0027.
Values may be sent and summed in bfloat16 or wider, within the bound.
A program may use at most 128 MiB of HBM per device.

```python
import math
import jax
import jax.numpy as jnp
from jax import lax

C = 512
NODE_DEV = 4096
TILE = 128
BLK = 8
SLOTS = 2
ITERS = 2
NODES = 524288
N_NODE = 128


def draw_far_count(key, part):
    first_key, second_key = jax.random.split(jax.random.fold_in(key, 17))
    counts = jax.random.randint(first_key, (N_NODE, N_NODE), 0, SLOTS + 1)
    busiest = jax.random.randint(second_key, (), 0, N_NODE)
    row_ids = jnp.arange(N_NODE)[:, None]
    return jnp.where(row_ids == busiest, SLOTS, counts).astype(jnp.int32)


def set_ends(values, rng, smallest, top_value):
    dims = values.shape
    place = [jax.random.randint(jax.random.fold_in(rng, axis), (), 0, dims[axis]) for axis in range(len(dims))]
    values = values.at[tuple(place)].set(smallest)
    longest = dims.index(max(dims))
    place[longest] = (place[longest] + 1) % dims[longest]
    return values.at[tuple(place)].set(top_value)


def block_scale(own_key, dims, cuts, smallest, high):
    factor_of, own = 1.0, jax.random.fold_in(own_key, 6)
    for dim, parts in cuts:
        steps = jnp.exp(jax.random.uniform(jax.random.fold_in(own, dim), (parts,), jnp.float32, smallest / len(cuts), high / len(cuts)))
        factor_of = factor_of * jnp.repeat(steps, dims[dim] // parts).reshape([-1 if axis == dim else 1 for axis in range(len(dims))])
    return factor_of


def normal_values(own_key, shape, width, most, pieces=(), dtype=jnp.bfloat16):
    array = width * jax.random.normal(own_key, shape, jnp.float32)
    if pieces:
        array = array * block_scale(own_key, shape, pieces, -0.22, 0.18)
    return jnp.clip(array, -most, most).astype(dtype)


def setup_inputs(seed: int = 0) -> dict:
    key_of = jax.random.split(jax.random.key(seed), 8)
    return {
        "labels": normal_values(key_of[0], (NODES, C), 1.0, 6.0, ((0, 128),)),
        "seed_mask": set_ends((jax.random.randint(key_of[1], (NODES,), 0, 4) < 1).astype(jnp.int32), jax.random.fold_in(key_of[1], 1), 0, 1),
        "band_w": jnp.clip(jnp.exp(math.log(1.0) - 6.9083047 * jax.random.uniform(key_of[2], (NODES // TILE, 3, TILE, TILE), jnp.float32) ** block_scale(key_of[2], (NODES // TILE, 3, TILE, TILE), ((0, 128),), -0.2, 0.2)), 0.0009994507, 1.0).astype(jnp.bfloat16),
        "far_block": set_ends(jax.random.randint(key_of[3], (N_NODE, N_NODE, SLOTS), 0, NODE_DEV // BLK), jax.random.fold_in(key_of[3], 1), 0, (NODE_DEV // BLK) - 1).astype(jnp.int32),
        "far_tile": set_ends(jax.random.randint(key_of[4], (N_NODE, N_NODE, SLOTS), 0, NODE_DEV // TILE), jax.random.fold_in(key_of[4], 1), 0, (NODE_DEV // TILE) - 1).astype(jnp.int32),
        "far_count": draw_far_count(jax.random.fold_in(key_of[7], 71), 0),
        "far_w": jnp.clip(jnp.exp(math.log(2.0) - 3.6927934 * jax.random.uniform(key_of[6], (N_NODE, N_NODE, SLOTS, BLK, TILE), jnp.float32) ** block_scale(key_of[6], (N_NODE, N_NODE, SLOTS, BLK, TILE), ((0, 128),), -0.2, 0.2)), 0.049804688, 2.0).astype(jnp.bfloat16),
    }


def live_table(count_row):
    return (jnp.arange(SLOTS)[None, :] < count_row[:, None]).astype(jnp.float32)

def reference(labels, seed_mask, band_w, far_block, far_tile, far_count, far_w):
    tile_total = labels.shape[0] // TILE
    block_count = NODE_DEV // BLK
    band_wide = band_w.astype(jnp.float32)
    degree_band = lax.optimization_barrier(jnp.sum(band_wide, axis=(1, 3)))

    def far_degree(packed):
        tiles_here, count_here, weight_here = packed
        live_weights = weight_here.astype(jnp.float32) * live_table(count_here)[:, :, None, None]
        weight_sums = lax.optimization_barrier(jnp.sum(live_weights, axis=2)).reshape(-1, TILE)
        return jnp.zeros((NODE_DEV // TILE, TILE), jnp.float32).at[tiles_here.reshape(-1)].add(weight_sums)
    degree_far = lax.map(far_degree, (far_tile, far_count, far_w)).reshape(tile_total, TILE)
    degree = degree_band + degree_far
    seeded = (seed_mask == 1).reshape(tile_total, TILE, 1)
    clamped = labels.astype(jnp.float32).reshape(tile_total, TILE, C)
    current = labels
    residuals = []
    for sweep in range(ITERS):
        tiles = current.astype(jnp.float32).reshape(tile_total, TILE, C)
        band_sum = jnp.zeros((tile_total, TILE, C), jnp.float32)
        for offset in (-1, 0, 1):
            source = jnp.roll(tiles, -offset, axis=0)
            band_sum = band_sum + jnp.einsum('itr,irc->itc', band_wide[:, offset + 1], source)
        blocks_all = current.reshape(N_NODE, block_count, BLK, C)

        def far_part(packed):
            wanted, tiles_here, count_here, weight_here = packed
            blocks = blocks_all[jnp.arange(N_NODE)[:, None], wanted].astype(jnp.float32)
            live_weights = weight_here.astype(jnp.float32) * live_table(count_here)[:, :, None, None]
            contrib = jnp.einsum('skqt,skqc->sktc', live_weights, blocks)
            return jnp.zeros((NODE_DEV // TILE, TILE, C), jnp.float32).at[tiles_here.reshape(-1)].add(contrib.reshape(-1, TILE, C))
        far_sum = lax.map(far_part, (far_block, far_tile, far_count, far_w)).reshape(tile_total, TILE, C)
        averaged = (band_sum + far_sum) / degree[:, :, None]
        row_scale = jnp.sqrt(lax.optimization_barrier(jnp.mean(averaged * averaged, axis=2, keepdims=True)))
        scaled = averaged / jnp.maximum(row_scale, 0.05)
        fresh = jnp.where(seeded, clamped, scaled).astype(jnp.bfloat16)
        residuals.append(lax.optimization_barrier(jnp.sum(jnp.abs(fresh.astype(jnp.float32) - tiles), axis=(1, 2))))
        current = fresh.reshape(labels.shape[0], C)
    return (current, jnp.stack(residuals))
```

```python
import functools
import itertools

import jax
import jax.numpy as jnp
import numpy as np
from jax import lax
from jax.experimental import pallas as pl
from jax.experimental.pallas import tpu as pltpu
from jax.sharding import PartitionSpec as P

MESH = pl.DeviceIdType.MESH
N = 128
TILES = 32
C = 512
F32 = jnp.float32
BF16 = jnp.bfloat16


def offset_order():
    chips = [c for c in itertools.product(range(4), repeat=3) if any(c)]
    hops = lambda c: sum(min(v, 4 - v) for v in c)
    seen, groups = set(), []
    for c in chips:
        if c in seen:
            continue
        group = set()
        for r in range(3):
            q = c[r:] + c[:r]
            group |= {q, tuple((-v) % 4 for v in q)}
        seen |= group
        groups.append(sorted(group))
    groups.sort(key=lambda g: -hops(g[0]))
    flat = [c for g in groups for c in g]
    order = [c + (1,) for c in flat] + [(0, 0, 0, 1)] + [c + (0,) for c in flat]
    return order + [(0, 0, 0, 0)]


ORDER = offset_order()
PIECES = ((0, 64), (64, 96), (96, 112), (112, 128))


def shifted(me, o):
    z = ((me >> 5) + o[0]) & 3
    x = ((me >> 3) + o[1]) & 3
    y = ((me >> 1) + o[2]) & 3
    return (z << 5) | (x << 3) | (y << 1) | ((me & 1) ^ o[3])


def back(o):
    return tuple((-v) % 4 for v in o[:3]) + (o[3],)


def kernel(
    labels, seed, band, wants, tiles, counts, far_w, code, out, res,
    lab, new, edge, bw, fw, wr, wt, tv, acc, deg, mask, ask, asked, flip, picks, send, got1, got2, rsum,
    load_sem, ask_send, ask_recv, pick_sem, send_sem, got_sem, halo_send, halo_recv,
):
    me = lax.axis_index("node")
    right, left = (me + 1) & (N - 1), (me + N - 1) & (N - 1)

    loads = [
        pltpu.make_async_copy(labels, lab, load_sem.at[0]),
        pltpu.make_async_copy(band, bw, load_sem.at[1]),
        pltpu.make_async_copy(far_w, fw, load_sem.at[2]),
    ]
    for copy in loads:
        copy.start()

    barrier = pltpu.get_barrier_semaphore()
    for o in ORDER[:-1]:
        pl.semaphore_signal(barrier, inc=1, device_id=(shifted(me, o),), device_id_type=MESH)

    flip[...] = jnp.zeros((N, N), jnp.int32)
    flip[0:2, :] = wants[...]
    ask[...] = jnp.transpose(flip[...]).reshape(N, 1, N)

    ones = jnp.ones((384, N), BF16)
    loads[0].wait()
    loads[1].wait()

    def band_lhs(t):
        return jnp.concatenate([bw[t, 0], bw[t, 1], bw[t, 2]], axis=1)

    def band_tile(cur, t):
        rows = pl.ds(pl.multiple_of(t * 128, 128), 128)
        around = cur[pl.ds(pl.multiple_of((t - 1) * 16, 16), 48)].reshape(384, C)
        acc[rows, :] = jnp.dot(band_lhs(t), around, preferred_element_type=F32)

    def band_ends(cur, sweep):
        low = jnp.concatenate([edge[2 * sweep], cur[0:32]], axis=0).reshape(384, C)
        acc[0:128, :] = jnp.dot(band_lhs(0), low, preferred_element_type=F32)
        high = jnp.concatenate([cur[TILES * 16 - 32 :], edge[2 * sweep + 1]], axis=0).reshape(384, C)
        acc[(TILES - 1) * 128 :, :] = jnp.dot(band_lhs(TILES - 1), high, preferred_element_type=F32)

    def first_band(t, carry):
        band_tile(lab, t)
        return carry

    lax.fori_loop(1, TILES - 1, first_band, 0)

    pl.semaphore_wait(barrier, N - 1)

    for j, o in enumerate(ORDER[:-1]):
        peer = shifted(me, o)
        pltpu.make_async_remote_copy(
            src_ref=ask.at[peer], dst_ref=asked.at[j], send_sem=ask_send, recv_sem=ask_recv,
            device_id=(peer,), device_id_type=MESH,
        ).start()

    def halo(cur, sweep):
        return [
            pltpu.make_async_remote_copy(
                src_ref=cur.at[pl.ds((TILES - 1) * 16, 16)], dst_ref=edge.at[2 * sweep],
                send_sem=halo_send.at[2 * sweep], recv_sem=halo_recv.at[2 * sweep],
                device_id=(right,), device_id_type=MESH,
            ),
            pltpu.make_async_remote_copy(
                src_ref=cur.at[pl.ds(0, 16)], dst_ref=edge.at[2 * sweep + 1],
                send_sem=halo_send.at[2 * sweep + 1], recv_sem=halo_recv.at[2 * sweep + 1],
                device_id=(left,), device_id_type=MESH,
            ),
        ]

    halo1 = halo(lab, 0)
    for copy in halo1:
        copy.start()
    asked[N - 1] = ask[me]

    loads[2].wait()
    for j, o in enumerate(ORDER):
        wr[16 * j : 16 * (j + 1), :] = fw[shifted(me, o)].reshape(16, N)
    for j in range(0, 2048, 128):
        wt[:, j : j + 128] = jnp.transpose(wr[j : j + 128, :].astype(F32)).astype(BF16)
    slot = lax.broadcasted_iota(jnp.int32, (2, N), 0)
    goal = jnp.where(slot < counts[...], tiles[...], 64).astype(F32).astype(BF16)
    goal = jnp.concatenate([goal, jnp.zeros((14, N), BF16)], axis=0)
    o = code[...]
    source = (
        ((((me >> 5) + (o >> 5)) & 3) << 5)
        | ((((me >> 3) + (o >> 3)) & 3) << 3)
        | ((((me >> 1) + (o >> 1)) & 3) << 1)
        | ((me ^ o) & 1)
    )
    spread = (lax.broadcasted_iota(jnp.int32, (N, 2048), 0) == source).astype(F32).astype(BF16)
    both = jnp.dot(goal, spread, preferred_element_type=F32)
    second = ((lax.broadcasted_iota(jnp.int32, (1, 2048), 1) >> 3) & 1) == 1
    tv[...] = jnp.where(second, both[1:2], both[0:1]).astype(jnp.int32)

    def far_lhs(p, j0, j1):
        w = wt[:, 16 * j0 : 16 * j1]
        to = tv[:, 16 * j0 : 16 * j1]
        parts = [w * (to == 2 * p + i).astype(F32).astype(BF16) for i in range(2)]
        return jnp.concatenate(parts, axis=0)

    def prepare(p, carry):
        rows = pl.ds(pl.multiple_of(p * 256, 256), 256)
        total = jnp.dot(far_lhs(p, 0, N), jnp.ones((2048, N), BF16), preferred_element_type=F32)
        bands = jnp.concatenate([band_lhs(2 * p), band_lhs(2 * p + 1)], axis=0)
        deg[rows, :] = 0.05 * (total + jnp.dot(bands, ones, preferred_element_type=F32))
        for i in range(2):
            row = seed[pl.ds(2 * p + i, 1), :].astype(F32)
            square = jnp.broadcast_to(row, (N, N))
            start = pl.multiple_of(p * 256 + i * 128, 128)
            mask[pl.ds(start, 128), :] = jnp.transpose(square)
        return carry

    lax.fori_loop(0, TILES // 2, prepare, 0)

    pltpu.make_async_copy(asked.at[pl.ds(0, N - 1)], asked.at[pl.ds(0, N - 1)], ask_recv).wait()
    flip[...] = jnp.transpose(asked[...].reshape(N, N))
    to_scalars = pltpu.make_async_copy(flip.at[pl.ds(0, 8)], picks, pick_sem)
    to_scalars.start()
    to_scalars.wait()

    def piece_of(j):
        return [i for i, (a, b) in enumerate(PIECES) if a <= j < b][0]

    def push(cur, got, sweep):
        def gather(lo, hi):
            def one(j, carry):
                for k in range(2):
                    send[2 * j + k] = cur[picks[k, j]]
                return carry

            lax.fori_loop(lo, hi, one, 0, unroll=4)

        def start(lo, hi):
            for j in range(lo, hi):
                pltpu.make_async_remote_copy(
                    src_ref=send.at[pl.ds(2 * j, 2)], dst_ref=got.at[pl.ds(2 * j, 2)],
                    send_sem=send_sem.at[sweep], recv_sem=got_sem.at[4 * sweep + piece_of(j)],
                    device_id=(shifted(me, back(ORDER[j])),), device_id_type=MESH,
                ).start()

        for k in range(2):
            got[2 * (N - 1) + k] = cur[picks[k, N - 1]]
        gather(0, 32)
        gather(32, 64)
        start(0, 32)
        gather(64, 96)
        start(32, 64)
        gather(96, 127)
        start(64, 127)

    def take(got, sweep, i):
        j0, j1 = PIECES[i]
        part = got.at[pl.ds(2 * j0, 2 * (min(j1, N - 1) - j0))]
        pltpu.make_async_copy(part, part, got_sem.at[4 * sweep + i]).wait()

    def far_piece(got, i, p):
        j0, j1 = PIECES[i]
        rhs = got[2 * j0 : 2 * j1].reshape(16 * (j1 - j0), C)
        return jnp.dot(far_lhs(p, j0, j1), rhs, preferred_element_type=F32)

    def sweep_far(got, sweep, finish):
        for i in range(len(PIECES) - 1):
            take(got, sweep, i)

            def add(p, carry):
                rows = pl.ds(pl.multiple_of(p * 256, 256), 256)
                acc[rows, :] = acc[rows, :] + far_piece(got, i, p)
                return carry

            lax.fori_loop(0, TILES // 2, add, 0)
        last = len(PIECES) - 1
        take(got, sweep, last)

        def end(p, carry):
            rows = pl.ds(pl.multiple_of(p * 256, 256), 256)
            x = acc[rows, :] + far_piece(got, last, p)
            square = jnp.sum(x * x, axis=1, keepdims=True)
            low = deg[rows, :]
            scale = 1.0 / jnp.maximum(jnp.sqrt(square * (1.0 / C)), low)
            scaled = x * jnp.concatenate([scale] * 4, axis=1)
            m = mask[rows, :]
            keep = jnp.concatenate([m] * 4, axis=1) == 1.0
            start = lab[pl.ds(pl.multiple_of(p * 32, 32), 32)].reshape(256, C)
            fresh = jnp.where(keep, start.astype(F32), scaled).astype(BF16)
            finish(p, fresh)
            return carry

        lax.fori_loop(0, TILES // 2, end, 0)

    def change(sweep, p, fresh, before):
        moved = jnp.abs(fresh.astype(F32) - before.astype(F32))
        for i in range(2):
            part = moved[128 * i : 128 * (i + 1)]
            lanes = part[:, 0:128] + part[:, 128:256] + part[:, 256:384] + part[:, 384:512]
            rsum[sweep * TILES + 2 * p + i] = jnp.sum(lanes.reshape(16, 8, 128), axis=0)

    push(lab, got1, 0)
    for copy in halo1:
        copy.wait()
    band_ends(lab, 0)

    def keep_new(p, fresh):
        new[pl.ds(pl.multiple_of(p * 32, 32), 32)] = fresh.reshape(32, 8, C)

    sweep_far(got1, 0, keep_new)

    sent = send.at[pl.ds(0, 2 * (N - 1))]
    pltpu.make_async_copy(sent, sent, send_sem.at[0]).wait()
    push(new, got2, 1)
    halo2 = halo(new, 1)
    for copy in halo2:
        copy.start()

    def second_band(t, carry):
        band_tile(new, t)
        return carry

    lax.fori_loop(1, TILES - 1, second_band, 0)

    def first_change(p, carry):
        block = pl.ds(pl.multiple_of(p * 32, 32), 32)
        change(0, p, new[block].reshape(256, C), lab[block].reshape(256, C))
        return carry

    lax.fori_loop(0, TILES // 2, first_change, 0)
    for copy in halo2:
        copy.wait()
    band_ends(new, 1)

    def keep_out(p, fresh):
        rows = pl.ds(pl.multiple_of(p * 256, 256), 256)
        out[rows, :] = fresh
        block = pl.ds(pl.multiple_of(p * 32, 32), 32)
        change(1, p, fresh, new[block].reshape(256, C))

    sweep_far(got2, 1, keep_out)
    res[...] = jnp.sum(jnp.sum(rsum[...], axis=1), axis=1, keepdims=True)

    pltpu.make_async_copy(sent, sent, send_sem.at[1]).wait()
    rows_sent = asked.at[pl.ds(0, N - 1)]
    pltpu.make_async_copy(rows_sent, rows_sent, ask_send).wait()


def body(labels, seed_mask, band_w, far_block, far_tile, far_count, far_w):
    code = np.array([(o[0] << 5) | (o[1] << 3) | (o[2] << 1) | o[3] for o in ORDER], np.int32)
    vmem = pl.BlockSpec(memory_space=pltpu.VMEM)
    hbm = pl.BlockSpec(memory_space=pl.ANY)
    dma = pltpu.SemaphoreType.DMA
    out, res = pl.pallas_call(
        kernel,
        out_shape=(
            jax.ShapeDtypeStruct((TILES * 128, C), BF16),
            jax.ShapeDtypeStruct((2 * TILES, 1), F32),
        ),
        in_specs=[hbm, vmem, hbm, vmem, vmem, vmem, hbm, vmem],
        out_specs=(vmem, vmem),
        scratch_shapes=[
            pltpu.VMEM((TILES * 16, 8, C), BF16),
            pltpu.VMEM((TILES * 16, 8, C), BF16),
            pltpu.VMEM((4, 16, 8, C), BF16),
            pltpu.VMEM((TILES, 3, 128, 128), BF16),
            pltpu.VMEM((N, 2, 8, 128), BF16),
            pltpu.VMEM((2048, 128), BF16),
            pltpu.VMEM((128, 2048), BF16),
            pltpu.VMEM((1, 2048), jnp.int32),
            pltpu.VMEM((TILES * 128, C), F32),
            pltpu.VMEM((TILES * 128, 128), F32),
            pltpu.VMEM((TILES * 128, 128), F32),
            pltpu.VMEM((N, 1, N), jnp.int32),
            pltpu.VMEM((N, 1, N), jnp.int32),
            pltpu.VMEM((N, N), jnp.int32),
            pltpu.SMEM((8, N), jnp.int32),
            pltpu.VMEM((2 * N, 8, C), BF16),
            pltpu.VMEM((2 * N, 8, C), BF16),
            pltpu.VMEM((2 * N, 8, C), BF16),
            pltpu.VMEM((2 * TILES, 8, 128), F32),
            dma((3,)), dma, dma, dma, dma((2,)), dma((8,)), dma((4,)), dma((4,)),
        ],
        compiler_params=pltpu.CompilerParams(
            collective_id=0, has_side_effects=True, vmem_limit_bytes=48 << 20
        ),
    )(
        labels.reshape(TILES * 16, 8, C),
        seed_mask.reshape(TILES, 128),
        band_w,
        jnp.swapaxes(far_block, 1, 2)[0],
        jnp.swapaxes(far_tile, 1, 2)[0],
        far_count,
        far_w[0],
        jnp.asarray(np.repeat(code, 16)[None]),
    )
    return out, res.reshape(2, TILES)


def solution(mesh):
    placed = (
        P("node", None),
        P("node"),
        P("node", None, None, None),
        P("node", None, None),
        P("node", None, None),
        P("node", None),
        P("node", None, None, None, None),
    )
    return jax.shard_map(
        body,
        mesh=mesh,
        in_specs=placed,
        out_specs=(P("node", None), P(None, "node")),
        check_vma=False,
    )
```

```python
import functools
import itertools

import jax
import jax.numpy as jnp
import numpy as np
from jax import lax
from jax.experimental import pallas as pl
from jax.experimental.pallas import tpu as pltpu
from jax.sharding import PartitionSpec as P

MESH = pl.DeviceIdType.MESH
N = 128
TILES = 32
C = 512
F32 = jnp.float32
BF16 = jnp.bfloat16


GROUPS = (
    (4, 5, 37, 47, 26, 50, 63, 28),
    (17, 10, 44, 2, 9, 36, 59, 35),
    (7, 40, 33, 12, 1, 38, 42, 15),
    (3, 20, 13, 25, 46, 34, 55, 56),
    (53, 18, 24, 11, 52, 45, 62, 19),
    (60, 6, 61, 16, 31, 54, 23, 41),
    (48, 21, 14, 8, 32, 58, 30, 39),
    (51, 22, 29, 43, 57, 49, 27, 0),
)
SIZE = 16
AHEAD = 4
PASSES = ((0, 2), (2, 4), (4, 6), (6, 8))
WIDE = 4
ADD_UNROLL = 2
END_UNROLL = 2
BAND_UNROLL = 2


def offset_order():
    hops = lambda v: sum(min(d, 4 - d) for d in (v >> 4, (v >> 2) & 3, v & 3))
    order = []
    for group in GROUPS:
        for v in sorted(group, key=lambda v: -hops(v)):
            order += [(v >> 4, (v >> 2) & 3, v & 3, c) for c in (1, 0)]
    return order


ORDER = offset_order()


def shifted(me, o):
    z = ((me >> 5) + o[0]) & 3
    x = ((me >> 3) + o[1]) & 3
    y = ((me >> 1) + o[2]) & 3
    return (z << 5) | (x << 3) | (y << 1) | ((me & 1) ^ o[3])


def back(o):
    return tuple((-v) % 4 for v in o[:3]) + (o[3],)


def kernel(
    labels, seed_in, band, wants_in, tiles_in, counts_in, far_w, code_in, out, res,
    seed, wants, tiles, counts, code, lab, new, edge, bw, fw, wr, wt, tv, acc, deg, mask, ask, asked, flip, picks, send, got1, got2, rsum, far_deg,
    load_sem, ask_send, ask_recv, pick_sem, send_sem, got_sem, halo_send, halo_recv,
):
    me = lax.axis_index("node")
    right, left = (me + 1) & (N - 1), (me + N - 1) & (N - 1)

    loads = [
        pltpu.make_async_copy(wants_in, wants, load_sem.at[0]),
        pltpu.make_async_copy(labels, lab, load_sem.at[1]),
        pltpu.make_async_copy(band, bw, load_sem.at[2]),
        pltpu.make_async_copy(far_w, fw, load_sem.at[3]),
        pltpu.make_async_copy(tiles_in, tiles, load_sem.at[4]),
        pltpu.make_async_copy(counts_in, counts, load_sem.at[5]),
        pltpu.make_async_copy(seed_in, seed, load_sem.at[6]),
        pltpu.make_async_copy(code_in, code, load_sem.at[7]),
    ]
    for copy in loads:
        copy.start()

    barrier = pltpu.get_barrier_semaphore()
    for o in ORDER[:-1]:
        pl.semaphore_signal(barrier, inc=1, device_id=(shifted(me, o),), device_id_type=MESH)

    loads[0].wait()
    flip[...] = jnp.zeros((N, N), jnp.int32)
    flip[0:2, :] = wants[...]
    ask[...] = jnp.transpose(flip[...]).reshape(N, 1, N)

    ones = jnp.ones((384, N), BF16)

    def band_lhs(t):
        return jnp.concatenate([bw[t, 0], bw[t, 1], bw[t, 2]], axis=1)

    def band_tile(cur, t):
        rows = pl.ds(pl.multiple_of(t * 128, 128), 128)
        around = cur[pl.ds(pl.multiple_of((t - 1) * 16, 16), 48)].reshape(384, C)
        acc[rows, :] = jnp.dot(band_lhs(t), around, preferred_element_type=F32)

    def band_ends(cur):
        low = jnp.concatenate([bw[0, 1], bw[0, 2]], axis=1)
        acc[0:128, :] = jnp.dot(low, cur[0:32].reshape(256, C), preferred_element_type=F32)
        high = jnp.concatenate([bw[TILES - 1, 0], bw[TILES - 1, 1]], axis=1)
        around = cur[TILES * 16 - 32 :].reshape(256, C)
        acc[(TILES - 1) * 128 :, :] = jnp.dot(high, around, preferred_element_type=F32)

    def add_edges(halos, sweep):
        for copy in halos:
            copy.wait()
        for rows, w, side in ((slice(0, 128), bw[0, 0], 0), (slice(TILES * 128 - 128, None), bw[TILES - 1, 2], 1)):
            part = edge[2 * sweep + side].reshape(128, C)
            acc[rows, :] = acc[rows, :] + jnp.dot(w, part, preferred_element_type=F32)

    def first_band(t, carry):
        band_tile(lab, t)
        return carry

    pl.semaphore_wait(barrier, N - 1)

    for j, o in enumerate(ORDER[:-1]):
        peer = shifted(me, o)
        pltpu.make_async_remote_copy(
            src_ref=ask.at[peer], dst_ref=asked.at[j], send_sem=ask_send, recv_sem=ask_recv,
            device_id=(peer,), device_id_type=MESH,
        ).start()

    def halo(cur, sweep):
        return [
            pltpu.make_async_remote_copy(
                src_ref=cur.at[pl.ds((TILES - 1) * 16, 16)], dst_ref=edge.at[2 * sweep],
                send_sem=halo_send.at[2 * sweep], recv_sem=halo_recv.at[2 * sweep],
                device_id=(right,), device_id_type=MESH,
            ),
            pltpu.make_async_remote_copy(
                src_ref=cur.at[pl.ds(0, 16)], dst_ref=edge.at[2 * sweep + 1],
                send_sem=halo_send.at[2 * sweep + 1], recv_sem=halo_recv.at[2 * sweep + 1],
                device_id=(left,), device_id_type=MESH,
            ),
        ]

    loads[1].wait()
    halo1 = halo(lab, 0)
    for copy in halo1:
        copy.start()
    asked[N - 1] = ask[me]

    for copy in loads[2:]:
        copy.wait()
    for j, o in enumerate(ORDER):
        wr[16 * j : 16 * (j + 1), :] = fw[shifted(me, o)].reshape(16, N)
    for j in range(0, 2048, 128):
        wt[:, j : j + 128] = jnp.transpose(wr[j : j + 128, :].astype(F32)).astype(BF16)
    slot = lax.broadcasted_iota(jnp.int32, (2, N), 0)
    goal = jnp.where(slot < counts[...], tiles[...], 64).astype(F32).astype(BF16)
    goal = jnp.concatenate([goal, jnp.zeros((14, N), BF16)], axis=0)
    o = code[...]
    source = (
        ((((me >> 5) + (o >> 5)) & 3) << 5)
        | ((((me >> 3) + (o >> 3)) & 3) << 3)
        | ((((me >> 1) + (o >> 1)) & 3) << 1)
        | ((me ^ o) & 1)
    )
    spread = (lax.broadcasted_iota(jnp.int32, (N, 2304), 0) == source).astype(F32).astype(BF16)
    both = jnp.dot(goal, spread, preferred_element_type=F32)
    lane = lax.broadcasted_iota(jnp.int32, (1, 2304), 1)
    second = jnp.where(lane < 2048, lane >> 3, lane) & 1 == 1
    tv[...] = jnp.where(second, both[1:2], both[0:1]).astype(jnp.int32)

    def far_lhs(p, j0, j1, parts):
        w = wt[:, 16 * j0 : 16 * j1]
        to = tv[:, 16 * j0 : 16 * j1]
        return jnp.concatenate([w * (to == parts * p + i).astype(F32).astype(BF16) for i in range(parts)], axis=0)

    def prepare(t, carry):
        rows = pl.ds(pl.multiple_of(t * 128, 128), 128)
        bands = jnp.dot(band_lhs(t), ones, preferred_element_type=F32)
        far = jnp.transpose(jnp.broadcast_to(far_deg[pl.ds(t, 1), :], (N, N)))
        deg[rows, :] = 0.05 * (bands + far)
        mask[rows, :] = jnp.transpose(jnp.broadcast_to(seed[pl.ds(t, 1), :].astype(F32), (N, N)))
        return carry

    def prepare_all():
        slot_sums = jnp.sum(wr[...].reshape(2 * N, 8, N).astype(F32), axis=1)
        tile = lax.broadcasted_iota(jnp.int32, (TILES, 2 * N), 0)
        hit = (tv[:, 2048:2304] == tile).astype(F32)
        far_deg[...] = jnp.dot(hit, slot_sums, precision=lax.Precision.HIGHEST, preferred_element_type=F32)
        lax.fori_loop(0, TILES, prepare, 0, unroll=2)

    pltpu.make_async_copy(asked.at[pl.ds(0, N - 1)], asked.at[pl.ds(0, N - 1)], ask_recv).wait()
    flip[...] = jnp.transpose(asked[...].reshape(N, N))
    to_scalars = pltpu.make_async_copy(flip.at[pl.ds(0, 8)], picks, pick_sem)
    to_scalars.start()
    to_scalars.wait()

    def gather(cur, got, g):
        def one(j, carry):
            for k in range(2):
                send[2 * j + k] = cur[picks[k, j]]
            return carry

        last = g == len(GROUPS) - 1
        lax.fori_loop(g * SIZE, (g + 1) * SIZE - last, one, 0, unroll=4)
        if last:
            for k in range(2):
                got[2 * (N - 1) + k] = cur[picks[k, N - 1]]

    def start(got, sweep, g):
        for j in range(g * SIZE, min((g + 1) * SIZE, N - 1)):
            pltpu.make_async_remote_copy(
                src_ref=send.at[pl.ds(2 * j, 2)], dst_ref=got.at[pl.ds(2 * j, 2)],
                send_sem=send_sem.at[sweep], recv_sem=got_sem.at[8 * sweep + g],
                device_id=(shifted(me, back(ORDER[j])),), device_id_type=MESH,
            ).start()

    def push(cur, got, sweep):
        gather(cur, got, 0)
        for g in range(1, 8):
            gather(cur, got, g)
            if g <= AHEAD:
                start(got, sweep, g - 1)

    def take(got, sweep, g):
        part = got.at[pl.ds(2 * g * SIZE, 2 * (min((g + 1) * SIZE, N - 1) - g * SIZE))]
        pltpu.make_async_copy(part, part, got_sem.at[8 * sweep + g]).wait()
        if g + AHEAD < 8:
            start(got, sweep, g + AHEAD)

    def far_piece(got, g0, g1, p, parts):
        rhs = got[2 * SIZE * g0 : 2 * SIZE * g1].reshape(16 * SIZE * (g1 - g0), C)
        return jnp.dot(far_lhs(p, g0 * SIZE, g1 * SIZE, parts), rhs, preferred_element_type=F32)

    def far_add(got, g0, g1):
        def add(p, carry):
            rows = pl.ds(pl.multiple_of(p * 128 * WIDE, 128 * WIDE), 128 * WIDE)
            acc[rows, :] = acc[rows, :] + far_piece(got, g0, g1, p, WIDE)
            return carry

        lax.fori_loop(0, TILES // WIDE, add, 0, unroll=ADD_UNROLL)

    def sweep_far(got, sweep, finish, between):
        for g0, g1 in PASSES[:-1]:
            for g in range(g0, g1):
                take(got, sweep, g)
            far_add(got, g0, g1)
            if g1 in between:
                between[g1]()
        last = PASSES[-1]
        for g in range(*last):
            take(got, sweep, g)

        def end(p, carry):
            rows = pl.ds(pl.multiple_of(p * 256, 256), 256)
            x = acc[rows, :] + far_piece(got, *last, p, 2)
            square = jnp.sum(x * x, axis=1, keepdims=True)
            low = deg[rows, :]
            scale = 1.0 / jnp.maximum(jnp.sqrt(square * (1.0 / C)), low)
            scaled = x * jnp.concatenate([scale] * 4, axis=1)
            m = mask[rows, :]
            keep = jnp.concatenate([m] * 4, axis=1) == 1.0
            given = lab[pl.ds(pl.multiple_of(p * 32, 32), 32)].reshape(256, C)
            fresh = jnp.where(keep, given.astype(F32), scaled).astype(BF16)
            finish(p, fresh)
            return carry

        lax.fori_loop(0, TILES // 2, end, 0, unroll=END_UNROLL)

    def change(sweep, p, fresh, before):
        moved = jnp.abs(fresh.astype(F32) - before.astype(F32))
        for i in range(2):
            part = moved[128 * i : 128 * (i + 1)]
            lanes = part[:, 0:128] + part[:, 128:256] + part[:, 256:384] + part[:, 384:512]
            rsum[sweep * TILES + 2 * p + i] = jnp.sum(lanes.reshape(16, 8, 128), axis=0)

    push(lab, got1, 0)
    band_ends(lab)
    lax.fori_loop(1, TILES - 1, first_band, 0, unroll=BAND_UNROLL)

    def while_arriving_1():
        prepare_all()
        add_edges(halo1, 0)

    def keep_new(p, fresh):
        new[pl.ds(pl.multiple_of(p * 32, 32), 32)] = fresh.reshape(32, 8, C)

    sweep_far(got1, 0, keep_new, {4: while_arriving_1})

    sent = send.at[pl.ds(0, 2 * (N - 1))]
    pltpu.make_async_copy(sent, sent, send_sem.at[0]).wait()
    halo2 = halo(new, 1)
    for copy in halo2:
        copy.start()
    push(new, got2, 1)
    band_ends(new)

    def second_band(t, carry):
        band_tile(new, t)
        return carry

    lax.fori_loop(1, TILES - 1, second_band, 0, unroll=BAND_UNROLL)

    def first_change(p, carry):
        block = pl.ds(pl.multiple_of(p * 32, 32), 32)
        change(0, p, new[block].reshape(256, C), lab[block].reshape(256, C))
        return carry

    def while_arriving_2():
        lax.fori_loop(0, TILES // 2, first_change, 0)
        add_edges(halo2, 1)

    def keep_out(p, fresh):
        rows = pl.ds(pl.multiple_of(p * 256, 256), 256)
        out[rows, :] = fresh
        block = pl.ds(pl.multiple_of(p * 32, 32), 32)
        change(1, p, fresh, new[block].reshape(256, C))

    sweep_far(got2, 1, keep_out, {4: while_arriving_2})
    sums = jnp.concatenate([jnp.sum(rsum[...], axis=1), jnp.zeros((64, N), F32)], axis=0)
    row = jnp.sum(jnp.transpose(sums), axis=0, keepdims=True)
    res[0:1, :] = row[:, 0:TILES]
    res[1:2, :] = row[:, TILES : 2 * TILES]

    pltpu.make_async_copy(sent, sent, send_sem.at[1]).wait()
    rows_sent = asked.at[pl.ds(0, N - 1)]
    pltpu.make_async_copy(rows_sent, rows_sent, ask_send).wait()


def body(labels, seed_mask, band_w, far_block, far_tile, far_count, far_w):
    code = np.array([(o[0] << 5) | (o[1] << 3) | (o[2] << 1) | o[3] for o in ORDER], np.int32)
    vmem = pl.BlockSpec(memory_space=pltpu.VMEM)
    hbm = pl.BlockSpec(memory_space=pltpu.HBM)
    dma = pltpu.SemaphoreType.DMA
    out, res = pl.pallas_call(
        kernel,
        out_shape=(
            pltpu.VMEM((TILES * 128, C), BF16),
            pltpu.VMEM((2, TILES), F32),
        ),
        in_specs=[hbm] * 8,
        out_specs=(vmem, vmem),
        scratch_shapes=[
            pltpu.VMEM((TILES, 128), jnp.int32),
            pltpu.VMEM((2, N), jnp.int32),
            pltpu.VMEM((2, N), jnp.int32),
            pltpu.VMEM((1, N), jnp.int32),
            pltpu.VMEM((1, 2304), jnp.int32),
            pltpu.VMEM((TILES * 16, 8, C), BF16),
            pltpu.VMEM((TILES * 16, 8, C), BF16),
            pltpu.VMEM((4, 16, 8, C), BF16),
            pltpu.VMEM((TILES, 3, 128, 128), BF16),
            pltpu.VMEM((N, 2, 8, 128), BF16),
            pltpu.VMEM((2048, 128), BF16),
            pltpu.VMEM((128, 2048), BF16),
            pltpu.VMEM((1, 2304), jnp.int32),
            pltpu.VMEM((TILES * 128, C), F32),
            pltpu.VMEM((TILES * 128, 128), F32),
            pltpu.VMEM((TILES * 128, 128), F32),
            pltpu.VMEM((N, 1, N), jnp.int32),
            pltpu.VMEM((N, 1, N), jnp.int32),
            pltpu.VMEM((N, N), jnp.int32),
            pltpu.SMEM((8, N), jnp.int32),
            pltpu.VMEM((2 * N, 8, C), BF16),
            pltpu.VMEM((2 * N, 8, C), BF16),
            pltpu.VMEM((2 * N, 8, C), BF16),
            pltpu.VMEM((2 * TILES, 8, 128), F32),
            pltpu.VMEM((TILES, 128), F32),
            dma((8,)), dma, dma, dma, dma((2,)), dma((16,)), dma((4,)), dma((4,)),
        ],
        compiler_params=pltpu.CompilerParams(
            collective_id=0, has_side_effects=True, vmem_limit_bytes=48 << 20
        ),
    )(*[
        pltpu.with_memory_space_constraint(x, pltpu.HBM)
        for x in (
            labels.reshape(TILES * 16, 8, C),
            seed_mask.reshape(TILES, 128),
            band_w,
            jnp.swapaxes(far_block, 1, 2)[0],
            jnp.swapaxes(far_tile, 1, 2)[0],
            far_count,
            far_w[0],
            jnp.asarray(np.concatenate([np.repeat(code, 16), np.repeat(code, 2)])[None]),
        )
    ])
    return out, res


def solution(mesh):
    placed = (
        P("node", None),
        P("node"),
        P("node", None, None, None),
        P("node", None, None),
        P("node", None, None),
        P("node", None),
        P("node", None, None, None, None),
    )
    return jax.shard_map(
        body,
        mesh=mesh,
        in_specs=placed,
        out_specs=(P("node", None), P(None, "node")),
        check_vma=False,
    )
```

```python
import functools
import itertools

import jax
import jax.numpy as jnp
import numpy as np
from jax import lax
from jax.experimental import pallas as pl
from jax.experimental.pallas import tpu as pltpu
from jax.sharding import PartitionSpec as P

MESH = pl.DeviceIdType.MESH
N = 128
TILES = 32
C = 512
F32 = jnp.float32
BF16 = jnp.bfloat16


GROUPS = (
    (4, 5, 37, 47, 26, 50, 63, 28),
    (17, 10, 44, 2, 9, 36, 59, 35),
    (7, 40, 33, 12, 1, 38, 42, 15),
    (3, 20, 13, 25, 46, 34, 55, 56),
    (53, 18, 24, 11, 52, 45, 62, 19),
    (60, 6, 61, 16, 31, 54, 23, 41),
    (48, 21, 14, 8, 32, 58, 30, 39),
    (51, 22, 29, 43, 57, 49, 27, 0),
)
SIZE = 16
AHEAD = (6, 6)
PASSES = ((0, 2), (2, 4), (4, 6), (6, 8))
WIDE = 4
ADD_UNROLL = 2
END_UNROLL = 4
BAND_UNROLL = 2


def offset_order():
    hops = lambda v: sum(min(d, 4 - d) for d in (v >> 4, (v >> 2) & 3, v & 3))
    order = []
    for group in GROUPS:
        for v in sorted(group, key=lambda v: -hops(v)):
            order += [(v >> 4, (v >> 2) & 3, v & 3, c) for c in (1, 0)]
    return order


ORDER = offset_order()


def shifted(me, o):
    z = ((me >> 5) + o[0]) & 3
    x = ((me >> 3) + o[1]) & 3
    y = ((me >> 1) + o[2]) & 3
    return (z << 5) | (x << 3) | (y << 1) | ((me & 1) ^ o[3])


def back(o):
    return tuple((-v) % 4 for v in o[:3]) + (o[3],)


def kernel(
    labels, seed_in, band, wants_in, tiles_in, counts_in, far_w, code_in, out, res,
    seed, wants, tiles, counts, code, lab, new, edge, bw, fw, wr, wt, tv, acc, deg, mask, ask, asked, flip, picks, send, got1, got2, rsum, far_deg,
    load_sem, ask_send, ask_recv, pick_sem, send_sem, got_sem, halo_send, halo_recv,
):
    me = lax.axis_index("node")
    right, left = (me + 1) & (N - 1), (me + N - 1) & (N - 1)

    loads = [
        pltpu.make_async_copy(wants_in, wants, load_sem.at[0]),
        pltpu.make_async_copy(labels, lab, load_sem.at[1]),
        pltpu.make_async_copy(band, bw, load_sem.at[2]),
        pltpu.make_async_copy(far_w, fw, load_sem.at[3]),
        pltpu.make_async_copy(tiles_in, tiles, load_sem.at[4]),
        pltpu.make_async_copy(counts_in, counts, load_sem.at[5]),
        pltpu.make_async_copy(seed_in, seed, load_sem.at[6]),
        pltpu.make_async_copy(code_in, code, load_sem.at[7]),
    ]
    for copy in loads:
        copy.start()

    barrier = pltpu.get_barrier_semaphore()
    for o in ORDER[:-1]:
        pl.semaphore_signal(barrier, inc=1, device_id=(shifted(me, o),), device_id_type=MESH)

    loads[0].wait()
    flip[...] = jnp.zeros((N, N), jnp.int32)
    flip[0:2, :] = wants[...]
    ask[...] = jnp.transpose(flip[...]).reshape(N, 1, N)

    ones = jnp.ones((384, N), BF16)

    def band_lhs(t):
        return jnp.concatenate([bw[t, 0], bw[t, 1], bw[t, 2]], axis=1)

    def band_tile(cur, t):
        rows = pl.ds(pl.multiple_of(t * 128, 128), 128)
        around = cur[pl.ds(pl.multiple_of((t - 1) * 16, 16), 48)].reshape(384, C)
        acc[rows, :] = jnp.dot(band_lhs(t), around, preferred_element_type=F32)

    def band_ends(cur):
        low = jnp.concatenate([bw[0, 1], bw[0, 2]], axis=1)
        acc[0:128, :] = jnp.dot(low, cur[0:32].reshape(256, C), preferred_element_type=F32)
        high = jnp.concatenate([bw[TILES - 1, 0], bw[TILES - 1, 1]], axis=1)
        around = cur[TILES * 16 - 32 :].reshape(256, C)
        acc[(TILES - 1) * 128 :, :] = jnp.dot(high, around, preferred_element_type=F32)

    def add_edges(halos, sweep):
        for copy in halos:
            copy.wait()
        for rows, w, side in ((slice(0, 128), bw[0, 0], 0), (slice(TILES * 128 - 128, None), bw[TILES - 1, 2], 1)):
            part = edge[2 * sweep + side].reshape(128, C)
            acc[rows, :] = acc[rows, :] + jnp.dot(w, part, preferred_element_type=F32)

    def first_band(t, carry):
        band_tile(lab, t)
        return carry

    pl.semaphore_wait(barrier, N - 1)

    for j, o in enumerate(ORDER[:-1]):
        peer = shifted(me, o)
        pltpu.make_async_remote_copy(
            src_ref=ask.at[peer], dst_ref=asked.at[j], send_sem=ask_send, recv_sem=ask_recv,
            device_id=(peer,), device_id_type=MESH,
        ).start()

    def halo(cur, sweep):
        return [
            pltpu.make_async_remote_copy(
                src_ref=cur.at[pl.ds((TILES - 1) * 16, 16)], dst_ref=edge.at[2 * sweep],
                send_sem=halo_send.at[2 * sweep], recv_sem=halo_recv.at[2 * sweep],
                device_id=(right,), device_id_type=MESH,
            ),
            pltpu.make_async_remote_copy(
                src_ref=cur.at[pl.ds(0, 16)], dst_ref=edge.at[2 * sweep + 1],
                send_sem=halo_send.at[2 * sweep + 1], recv_sem=halo_recv.at[2 * sweep + 1],
                device_id=(left,), device_id_type=MESH,
            ),
        ]

    loads[1].wait()
    halo1 = halo(lab, 0)
    for copy in halo1:
        copy.start()
    asked[N - 1] = ask[me]

    for copy in loads[2:]:
        copy.wait()
    for j, o in enumerate(ORDER):
        wr[16 * j : 16 * (j + 1), :] = fw[shifted(me, o)].reshape(16, N)
    for j in range(0, 2048, 128):
        wt[:, j : j + 128] = jnp.transpose(wr[j : j + 128, :].astype(F32)).astype(BF16)
    slot = lax.broadcasted_iota(jnp.int32, (2, N), 0)
    goal = jnp.where(slot < counts[...], tiles[...], 64).astype(F32).astype(BF16)
    goal = jnp.concatenate([goal, jnp.zeros((14, N), BF16)], axis=0)
    o = code[...]
    source = (
        ((((me >> 5) + (o >> 5)) & 3) << 5)
        | ((((me >> 3) + (o >> 3)) & 3) << 3)
        | ((((me >> 1) + (o >> 1)) & 3) << 1)
        | ((me ^ o) & 1)
    )
    spread = (lax.broadcasted_iota(jnp.int32, (N, 2304), 0) == source).astype(F32).astype(BF16)
    both = jnp.dot(goal, spread, preferred_element_type=F32)
    lane = lax.broadcasted_iota(jnp.int32, (1, 2304), 1)
    second = jnp.where(lane < 2048, lane >> 3, lane) & 1 == 1
    tv[...] = jnp.where(second, both[1:2], both[0:1]).astype(jnp.int32)

    def far_lhs(p, j0, j1, parts):
        w = wt[:, 16 * j0 : 16 * j1]
        to = tv[:, 16 * j0 : 16 * j1]
        return jnp.concatenate([w * (to == parts * p + i).astype(F32).astype(BF16) for i in range(parts)], axis=0)

    def prepare(t, carry):
        rows = pl.ds(pl.multiple_of(t * 128, 128), 128)
        bands = jnp.dot(band_lhs(t), ones, preferred_element_type=F32)
        far = jnp.transpose(jnp.broadcast_to(far_deg[pl.ds(t, 1), :], (N, N)))
        deg[rows, :] = 0.05 * (bands + far)
        mask[rows, :] = jnp.transpose(jnp.broadcast_to(seed[pl.ds(t, 1), :].astype(F32), (N, N)))
        return carry

    def prepare_all():
        slot_sums = jnp.sum(wr[...].reshape(2 * N, 8, N).astype(F32), axis=1)
        tile = lax.broadcasted_iota(jnp.int32, (TILES, 2 * N), 0)
        hit = (tv[:, 2048:2304] == tile).astype(F32)
        far_deg[...] = jnp.dot(hit, slot_sums, precision=lax.Precision.HIGHEST, preferred_element_type=F32)
        lax.fori_loop(0, TILES, prepare, 0, unroll=2)

    pltpu.make_async_copy(asked.at[pl.ds(0, N - 1)], asked.at[pl.ds(0, N - 1)], ask_recv).wait()
    flip[...] = jnp.transpose(asked[...].reshape(N, N))
    to_scalars = pltpu.make_async_copy(flip.at[pl.ds(0, 8)], picks, pick_sem)
    to_scalars.start()
    to_scalars.wait()

    def gather(cur, got, g):
        def one(j, carry):
            for k in range(2):
                send[2 * j + k] = cur[picks[k, j]]
            return carry

        last = g == len(GROUPS) - 1
        lax.fori_loop(g * SIZE, (g + 1) * SIZE - last, one, 0, unroll=4)
        if last:
            for k in range(2):
                got[2 * (N - 1) + k] = cur[picks[k, N - 1]]

    def start(got, sweep, g):
        for j in range(g * SIZE, min((g + 1) * SIZE, N - 1)):
            pltpu.make_async_remote_copy(
                src_ref=send.at[pl.ds(2 * j, 2)], dst_ref=got.at[pl.ds(2 * j, 2)],
                send_sem=send_sem.at[sweep], recv_sem=got_sem.at[8 * sweep + g],
                device_id=(shifted(me, back(ORDER[j])),), device_id_type=MESH,
            ).start()

    def push(cur, got, sweep):
        gather(cur, got, 0)
        for g in range(1, 9):
            if g < 8:
                gather(cur, got, g)
            if g <= AHEAD[sweep]:
                start(got, sweep, g - 1)

    def take(got, sweep, g):
        part = got.at[pl.ds(2 * g * SIZE, 2 * (min((g + 1) * SIZE, N - 1) - g * SIZE))]
        pltpu.make_async_copy(part, part, got_sem.at[8 * sweep + g]).wait()
        if g + AHEAD[sweep] < 8:
            start(got, sweep, g + AHEAD[sweep])

    def far_piece(got, g0, g1, p, parts):
        rhs = got[2 * SIZE * g0 : 2 * SIZE * g1].reshape(16 * SIZE * (g1 - g0), C)
        return jnp.dot(far_lhs(p, g0 * SIZE, g1 * SIZE, parts), rhs, preferred_element_type=F32)

    def far_add(got, g0, g1):
        def add(p, carry):
            rows = pl.ds(pl.multiple_of(p * 128 * WIDE, 128 * WIDE), 128 * WIDE)
            acc[rows, :] = acc[rows, :] + far_piece(got, g0, g1, p, WIDE)
            return carry

        lax.fori_loop(0, TILES // WIDE, add, 0, unroll=ADD_UNROLL)

    def sweep_far(got, sweep, finish, between):
        for g0, g1 in PASSES[:-1]:
            for g in range(g0, g1):
                take(got, sweep, g)
            far_add(got, g0, g1)
            if g1 in between:
                between[g1]()
        last = PASSES[-1]
        for g in range(*last):
            take(got, sweep, g)

        def end(p, carry):
            rows = pl.ds(pl.multiple_of(p * 256, 256), 256)
            x = acc[rows, :] + far_piece(got, *last, p, 2)
            square = jnp.sum(x * x, axis=1, keepdims=True)
            low = deg[rows, :]
            scale = 1.0 / jnp.maximum(jnp.sqrt(square * (1.0 / C)), low)
            scaled = x * jnp.concatenate([scale] * 4, axis=1)
            m = mask[rows, :]
            keep = jnp.concatenate([m] * 4, axis=1) == 1.0
            given = lab[pl.ds(pl.multiple_of(p * 32, 32), 32)].reshape(256, C)
            fresh = jnp.where(keep, given.astype(F32), scaled).astype(BF16)
            finish(p, fresh)
            return carry

        lax.fori_loop(0, TILES // 2, end, 0, unroll=END_UNROLL)

    def change(sweep, p, fresh, before):
        moved = jnp.abs(fresh.astype(F32) - before.astype(F32))
        for i in range(2):
            part = moved[128 * i : 128 * (i + 1)]
            lanes = part[:, 0:128] + part[:, 128:256] + part[:, 256:384] + part[:, 384:512]
            rsum[sweep * TILES + 2 * p + i] = jnp.sum(lanes.reshape(16, 8, 128), axis=0)

    push(lab, got1, 0)
    band_ends(lab)
    lax.fori_loop(1, TILES - 1, first_band, 0, unroll=BAND_UNROLL)

    def while_arriving_1():
        prepare_all()
        add_edges(halo1, 0)

    def keep_new(p, fresh):
        new[pl.ds(pl.multiple_of(p * 32, 32), 32)] = fresh.reshape(32, 8, C)

    sweep_far(got1, 0, keep_new, {4: while_arriving_1})

    sent = send.at[pl.ds(0, 2 * (N - 1))]
    pltpu.make_async_copy(sent, sent, send_sem.at[0]).wait()
    halo2 = halo(new, 1)
    push(new, got2, 1)
    for copy in halo2:
        copy.start()
    band_ends(new)

    def second_band(t, carry):
        band_tile(new, t)
        return carry

    lax.fori_loop(1, TILES - 1, second_band, 0, unroll=BAND_UNROLL)

    def first_change(p, carry):
        block = pl.ds(pl.multiple_of(p * 32, 32), 32)
        change(0, p, new[block].reshape(256, C), lab[block].reshape(256, C))
        return carry

    def while_arriving_2():
        lax.fori_loop(0, TILES // 2, first_change, 0)
        add_edges(halo2, 1)

    def keep_out(p, fresh):
        rows = pl.ds(pl.multiple_of(p * 256, 256), 256)
        out[rows, :] = fresh
        block = pl.ds(pl.multiple_of(p * 32, 32), 32)
        change(1, p, fresh, new[block].reshape(256, C))

    sweep_far(got2, 1, keep_out, {4: while_arriving_2})
    sums = jnp.concatenate([jnp.sum(rsum[...], axis=1), jnp.zeros((64, N), F32)], axis=0)
    row = jnp.sum(jnp.transpose(sums), axis=0, keepdims=True)
    res[0:1, :] = row[:, 0:TILES]
    res[1:2, :] = row[:, TILES : 2 * TILES]

    pltpu.make_async_copy(sent, sent, send_sem.at[1]).wait()
    rows_sent = asked.at[pl.ds(0, N - 1)]
    pltpu.make_async_copy(rows_sent, rows_sent, ask_send).wait()


def body(labels, seed_mask, band_w, far_block, far_tile, far_count, far_w):
    code = np.array([(o[0] << 5) | (o[1] << 3) | (o[2] << 1) | o[3] for o in ORDER], np.int32)
    vmem = pl.BlockSpec(memory_space=pltpu.VMEM)
    hbm = pl.BlockSpec(memory_space=pltpu.HBM)
    dma = pltpu.SemaphoreType.DMA
    out, res = pl.pallas_call(
        kernel,
        out_shape=(
            pltpu.VMEM((TILES * 128, C), BF16),
            pltpu.VMEM((2, TILES), F32),
        ),
        in_specs=[hbm] * 8,
        out_specs=(vmem, vmem),
        scratch_shapes=[
            pltpu.VMEM((TILES, 128), jnp.int32),
            pltpu.VMEM((2, N), jnp.int32),
            pltpu.VMEM((2, N), jnp.int32),
            pltpu.VMEM((1, N), jnp.int32),
            pltpu.VMEM((1, 2304), jnp.int32),
            pltpu.VMEM((TILES * 16, 8, C), BF16),
            pltpu.VMEM((TILES * 16, 8, C), BF16),
            pltpu.VMEM((4, 16, 8, C), BF16),
            pltpu.VMEM((TILES, 3, 128, 128), BF16),
            pltpu.VMEM((N, 2, 8, 128), BF16),
            pltpu.VMEM((2048, 128), BF16),
            pltpu.VMEM((128, 2048), BF16),
            pltpu.VMEM((1, 2304), jnp.int32),
            pltpu.VMEM((TILES * 128, C), F32),
            pltpu.VMEM((TILES * 128, 128), F32),
            pltpu.VMEM((TILES * 128, 128), F32),
            pltpu.VMEM((N, 1, N), jnp.int32),
            pltpu.VMEM((N, 1, N), jnp.int32),
            pltpu.VMEM((N, N), jnp.int32),
            pltpu.SMEM((8, N), jnp.int32),
            pltpu.VMEM((2 * N, 8, C), BF16),
            pltpu.VMEM((2 * N, 8, C), BF16),
            pltpu.VMEM((2 * N, 8, C), BF16),
            pltpu.VMEM((2 * TILES, 8, 128), F32),
            pltpu.VMEM((TILES, 128), F32),
            dma((8,)), dma, dma, dma, dma((2,)), dma((16,)), dma((4,)), dma((4,)),
        ],
        compiler_params=pltpu.CompilerParams(
            collective_id=0, has_side_effects=True, vmem_limit_bytes=48 << 20
        ),
    )(*[
        pltpu.with_memory_space_constraint(x, pltpu.HBM)
        for x in (
            labels.reshape(TILES * 16, 8, C),
            seed_mask.reshape(TILES, 128),
            band_w,
            jnp.swapaxes(far_block, 1, 2)[0],
            jnp.swapaxes(far_tile, 1, 2)[0],
            far_count,
            far_w[0],
            jnp.asarray(np.concatenate([np.repeat(code, 16), np.repeat(code, 2)])[None]),
        )
    ])
    return out, res


def solution(mesh):
    placed = (
        P("node", None),
        P("node"),
        P("node", None, None, None),
        P("node", None, None),
        P("node", None, None),
        P("node", None),
        P("node", None, None, None, None),
    )
    return jax.shard_map(
        body,
        mesh=mesh,
        in_specs=placed,
        out_specs=(P("node", None), P(None, "node")),
        check_vma=False,
    )
```

```python
import functools
import itertools

import jax
import jax.numpy as jnp
import numpy as np
from jax import lax
from jax.experimental import pallas as pl
from jax.experimental.pallas import tpu as pltpu
from jax.sharding import PartitionSpec as P

MESH = pl.DeviceIdType.MESH
N = 128
TILES = 32
C = 512
F32 = jnp.float32
BF16 = jnp.bfloat16


GROUPS = (
    (4, 5, 37, 47, 26, 50, 63, 28),
    (17, 10, 44, 2, 9, 36, 59, 35),
    (7, 40, 33, 12, 1, 38, 42, 15),
    (3, 20, 13, 25, 46, 34, 55, 56),
    (53, 18, 24, 11, 52, 45, 62, 19),
    (60, 6, 61, 16, 31, 54, 23, 41),
    (48, 21, 14, 8, 32, 58, 30, 39),
    (51, 22, 29, 43, 57, 49, 27, 0),
)
SIZE = 16
AHEAD = (6, 6)
PASSES = ((0, 3), (3, 6), (6, 8))
WIDE = 4
ADD_UNROLL = 2
END_UNROLL = 4
BAND_UNROLL = 2


def offset_order():
    hops = lambda v: sum(min(d, 4 - d) for d in (v >> 4, (v >> 2) & 3, v & 3))
    order = []
    for group in GROUPS:
        for v in sorted(group, key=lambda v: -hops(v)):
            order += [(v >> 4, (v >> 2) & 3, v & 3, c) for c in (1, 0)]
    return order


ORDER = offset_order()


def shifted(me, o):
    z = ((me >> 5) + o[0]) & 3
    x = ((me >> 3) + o[1]) & 3
    y = ((me >> 1) + o[2]) & 3
    return (z << 5) | (x << 3) | (y << 1) | ((me & 1) ^ o[3])


def back(o):
    return tuple((-v) % 4 for v in o[:3]) + (o[3],)


def kernel(
    labels, seed_in, band, wants_in, tiles_in, counts_in, far_w, code_in, out, res,
    seed, wants, tiles, counts, code, lab, new, edge, bw, fw, wr, wt, tv, acc, deg, mask, ask, asked, flip, picks, send, got1, got2, rsum, far_deg,
    load_sem, ask_send, ask_recv, pick_sem, send_sem, got_sem, halo_send, halo_recv,
):
    me = lax.axis_index("node")
    right, left = (me + 1) & (N - 1), (me + N - 1) & (N - 1)

    loads = [
        pltpu.make_async_copy(wants_in, wants, load_sem.at[0]),
        pltpu.make_async_copy(labels, lab, load_sem.at[1]),
        pltpu.make_async_copy(band, bw, load_sem.at[2]),
        pltpu.make_async_copy(far_w, fw, load_sem.at[3]),
        pltpu.make_async_copy(tiles_in, tiles, load_sem.at[4]),
        pltpu.make_async_copy(counts_in, counts, load_sem.at[5]),
        pltpu.make_async_copy(seed_in, seed, load_sem.at[6]),
        pltpu.make_async_copy(code_in, code, load_sem.at[7]),
    ]
    for copy in loads:
        copy.start()

    barrier = pltpu.get_barrier_semaphore()
    for o in ORDER[:-1]:
        pl.semaphore_signal(barrier, inc=1, device_id=(shifted(me, o),), device_id_type=MESH)

    loads[0].wait()
    flip[...] = jnp.zeros((N, N), jnp.int32)
    flip[0:2, :] = wants[...]
    ask[...] = jnp.transpose(flip[...]).reshape(N, 1, N)

    ones = jnp.ones((384, N), BF16)

    def band_lhs(t):
        return jnp.concatenate([bw[t, 0], bw[t, 1], bw[t, 2]], axis=1)

    def band_tile(cur, t):
        rows = pl.ds(pl.multiple_of(t * 128, 128), 128)
        around = cur[pl.ds(pl.multiple_of((t - 1) * 16, 16), 48)].reshape(384, C)
        acc[rows, :] = jnp.dot(band_lhs(t), around, preferred_element_type=F32)

    def band_ends(cur):
        low = jnp.concatenate([bw[0, 1], bw[0, 2]], axis=1)
        acc[0:128, :] = jnp.dot(low, cur[0:32].reshape(256, C), preferred_element_type=F32)
        high = jnp.concatenate([bw[TILES - 1, 0], bw[TILES - 1, 1]], axis=1)
        around = cur[TILES * 16 - 32 :].reshape(256, C)
        acc[(TILES - 1) * 128 :, :] = jnp.dot(high, around, preferred_element_type=F32)

    def add_edges(halos, sweep):
        for copy in halos:
            copy.wait()
        for rows, w, side in ((slice(0, 128), bw[0, 0], 0), (slice(TILES * 128 - 128, None), bw[TILES - 1, 2], 1)):
            part = edge[2 * sweep + side].reshape(128, C)
            acc[rows, :] = acc[rows, :] + jnp.dot(w, part, preferred_element_type=F32)

    def first_band(t, carry):
        band_tile(lab, t)
        return carry

    pl.semaphore_wait(barrier, N - 1)

    for j, o in enumerate(ORDER[:-1]):
        peer = shifted(me, o)
        pltpu.make_async_remote_copy(
            src_ref=ask.at[peer], dst_ref=asked.at[j], send_sem=ask_send, recv_sem=ask_recv,
            device_id=(peer,), device_id_type=MESH,
        ).start()

    def halo(cur, sweep):
        return [
            pltpu.make_async_remote_copy(
                src_ref=cur.at[pl.ds((TILES - 1) * 16, 16)], dst_ref=edge.at[2 * sweep],
                send_sem=halo_send.at[2 * sweep], recv_sem=halo_recv.at[2 * sweep],
                device_id=(right,), device_id_type=MESH,
            ),
            pltpu.make_async_remote_copy(
                src_ref=cur.at[pl.ds(0, 16)], dst_ref=edge.at[2 * sweep + 1],
                send_sem=halo_send.at[2 * sweep + 1], recv_sem=halo_recv.at[2 * sweep + 1],
                device_id=(left,), device_id_type=MESH,
            ),
        ]

    loads[1].wait()
    halo1 = halo(lab, 0)
    for copy in halo1:
        copy.start()
    asked[N - 1] = ask[me]

    for copy in loads[2:]:
        copy.wait()
    for j, o in enumerate(ORDER):
        wr[16 * j : 16 * (j + 1), :] = fw[shifted(me, o)].reshape(16, N)
    for j in range(0, 2048, 128):
        wt[:, j : j + 128] = jnp.transpose(wr[j : j + 128, :].astype(F32)).astype(BF16)
    slot = lax.broadcasted_iota(jnp.int32, (2, N), 0)
    goal = jnp.where(slot < counts[...], tiles[...], 64).astype(F32).astype(BF16)
    goal = jnp.concatenate([goal, jnp.zeros((14, N), BF16)], axis=0)
    o = code[...]
    source = (
        ((((me >> 5) + (o >> 5)) & 3) << 5)
        | ((((me >> 3) + (o >> 3)) & 3) << 3)
        | ((((me >> 1) + (o >> 1)) & 3) << 1)
        | ((me ^ o) & 1)
    )
    spread = (lax.broadcasted_iota(jnp.int32, (N, 2304), 0) == source).astype(F32).astype(BF16)
    both = jnp.dot(goal, spread, preferred_element_type=F32)
    lane = lax.broadcasted_iota(jnp.int32, (1, 2304), 1)
    second = jnp.where(lane < 2048, lane >> 3, lane) & 1 == 1
    tv[...] = jnp.where(second, both[1:2], both[0:1]).astype(jnp.int32)

    def far_lhs(p, j0, j1, parts):
        w = wt[:, 16 * j0 : 16 * j1]
        to = tv[:, 16 * j0 : 16 * j1]
        return jnp.concatenate([w * (to == parts * p + i).astype(F32).astype(BF16) for i in range(parts)], axis=0)

    def prepare(t, carry):
        rows = pl.ds(pl.multiple_of(t * 128, 128), 128)
        bands = jnp.dot(band_lhs(t), ones, preferred_element_type=F32)
        far = jnp.transpose(jnp.broadcast_to(far_deg[pl.ds(t, 1), :], (N, N)))
        deg[rows, :] = 0.05 * (bands + far)
        mask[rows, :] = jnp.transpose(jnp.broadcast_to(seed[pl.ds(t, 1), :].astype(F32), (N, N)))
        return carry

    def prepare_all():
        slot_sums = jnp.sum(wr[...].reshape(2 * N, 8, N).astype(F32), axis=1)
        tile = lax.broadcasted_iota(jnp.int32, (TILES, 2 * N), 0)
        hit = (tv[:, 2048:2304] == tile).astype(F32)
        far_deg[...] = jnp.dot(hit, slot_sums, precision=lax.Precision.HIGHEST, preferred_element_type=F32)
        lax.fori_loop(0, TILES, prepare, 0, unroll=2)

    pltpu.make_async_copy(asked.at[pl.ds(0, N - 1)], asked.at[pl.ds(0, N - 1)], ask_recv).wait()
    flip[...] = jnp.transpose(asked[...].reshape(N, N))
    to_scalars = pltpu.make_async_copy(flip.at[pl.ds(0, 8)], picks, pick_sem)
    to_scalars.start()
    to_scalars.wait()

    def gather(cur, got, g):
        def one(j, carry):
            for k in range(2):
                send[2 * j + k] = cur[picks[k, j]]
            return carry

        last = g == len(GROUPS) - 1
        lax.fori_loop(g * SIZE, (g + 1) * SIZE - last, one, 0, unroll=4)
        if last:
            for k in range(2):
                got[2 * (N - 1) + k] = cur[picks[k, N - 1]]

    def start(got, sweep, g):
        for j in range(g * SIZE, min((g + 1) * SIZE, N - 1)):
            pltpu.make_async_remote_copy(
                src_ref=send.at[pl.ds(2 * j, 2)], dst_ref=got.at[pl.ds(2 * j, 2)],
                send_sem=send_sem.at[sweep], recv_sem=got_sem.at[8 * sweep + g],
                device_id=(shifted(me, back(ORDER[j])),), device_id_type=MESH,
            ).start()

    def push(cur, got, sweep):
        gather(cur, got, 0)
        for g in range(1, 9):
            if g < 8:
                gather(cur, got, g)
            if g <= AHEAD[sweep]:
                start(got, sweep, g - 1)

    def take(got, sweep, g):
        part = got.at[pl.ds(2 * g * SIZE, 2 * (min((g + 1) * SIZE, N - 1) - g * SIZE))]
        pltpu.make_async_copy(part, part, got_sem.at[8 * sweep + g]).wait()
        if g + AHEAD[sweep] < 8:
            start(got, sweep, g + AHEAD[sweep])

    def far_piece(got, g0, g1, p, parts):
        rhs = got[2 * SIZE * g0 : 2 * SIZE * g1].reshape(16 * SIZE * (g1 - g0), C)
        return jnp.dot(far_lhs(p, g0 * SIZE, g1 * SIZE, parts), rhs, preferred_element_type=F32)

    def far_add(got, g0, g1):
        def add(p, carry):
            rows = pl.ds(pl.multiple_of(p * 128 * WIDE, 128 * WIDE), 128 * WIDE)
            acc[rows, :] = acc[rows, :] + far_piece(got, g0, g1, p, WIDE)
            return carry

        lax.fori_loop(0, TILES // WIDE, add, 0, unroll=ADD_UNROLL)

    def sweep_far(got, sweep, finish, between):
        for g0, g1 in PASSES[:-1]:
            for g in range(g0, g1):
                take(got, sweep, g)
            far_add(got, g0, g1)
            if g1 in between:
                between[g1]()
        last = PASSES[-1]
        for g in range(*last):
            take(got, sweep, g)

        def end(p, carry):
            rows = pl.ds(pl.multiple_of(p * 256, 256), 256)
            x = acc[rows, :] + far_piece(got, *last, p, 2)
            square = jnp.sum(x * x, axis=1, keepdims=True)
            low = deg[rows, :]
            scale = 1.0 / jnp.maximum(jnp.sqrt(square * (1.0 / C)), low)
            scaled = x * jnp.concatenate([scale] * 4, axis=1)
            m = mask[rows, :]
            keep = jnp.concatenate([m] * 4, axis=1) == 1.0
            given = lab[pl.ds(pl.multiple_of(p * 32, 32), 32)].reshape(256, C)
            fresh = jnp.where(keep, given.astype(F32), scaled).astype(BF16)
            finish(p, fresh)
            return carry

        lax.fori_loop(0, TILES // 2, end, 0, unroll=END_UNROLL)

    def change(sweep, p, fresh, before):
        moved = jnp.abs(fresh.astype(F32) - before.astype(F32))
        for i in range(2):
            part = moved[128 * i : 128 * (i + 1)]
            lanes = part[:, 0:128] + part[:, 128:256] + part[:, 256:384] + part[:, 384:512]
            rsum[sweep * TILES + 2 * p + i] = jnp.sum(lanes.reshape(16, 8, 128), axis=0)

    push(lab, got1, 0)
    band_ends(lab)
    lax.fori_loop(1, TILES - 1, first_band, 0, unroll=BAND_UNROLL)

    prepare_all()

    def while_arriving_1():
        add_edges(halo1, 0)

    def keep_new(p, fresh):
        new[pl.ds(pl.multiple_of(p * 32, 32), 32)] = fresh.reshape(32, 8, C)

    sweep_far(got1, 0, keep_new, {3: while_arriving_1})

    sent = send.at[pl.ds(0, 2 * (N - 1))]
    pltpu.make_async_copy(sent, sent, send_sem.at[0]).wait()
    halo2 = halo(new, 1)
    push(new, got2, 1)
    for copy in halo2:
        copy.start()
    band_ends(new)

    def second_band(t, carry):
        band_tile(new, t)
        return carry

    lax.fori_loop(1, TILES - 1, second_band, 0, unroll=BAND_UNROLL)

    def first_change(p, carry):
        block = pl.ds(pl.multiple_of(p * 32, 32), 32)
        change(0, p, new[block].reshape(256, C), lab[block].reshape(256, C))
        return carry

    lax.fori_loop(0, TILES // 2, first_change, 0)

    def while_arriving_2():
        add_edges(halo2, 1)

    def keep_out(p, fresh):
        rows = pl.ds(pl.multiple_of(p * 256, 256), 256)
        out[rows, :] = fresh
        block = pl.ds(pl.multiple_of(p * 32, 32), 32)
        change(1, p, fresh, new[block].reshape(256, C))

    sweep_far(got2, 1, keep_out, {3: while_arriving_2})
    sums = jnp.concatenate([jnp.sum(rsum[...], axis=1), jnp.zeros((64, N), F32)], axis=0)
    row = jnp.sum(jnp.transpose(sums), axis=0, keepdims=True)
    res[0:1, :] = row[:, 0:TILES]
    res[1:2, :] = row[:, TILES : 2 * TILES]

    pltpu.make_async_copy(sent, sent, send_sem.at[1]).wait()
    rows_sent = asked.at[pl.ds(0, N - 1)]
    pltpu.make_async_copy(rows_sent, rows_sent, ask_send).wait()


def body(labels, seed_mask, band_w, far_block, far_tile, far_count, far_w):
    code = np.array([(o[0] << 5) | (o[1] << 3) | (o[2] << 1) | o[3] for o in ORDER], np.int32)
    vmem = pl.BlockSpec(memory_space=pltpu.VMEM)
    hbm = pl.BlockSpec(memory_space=pltpu.HBM)
    dma = pltpu.SemaphoreType.DMA
    out, res = pl.pallas_call(
        kernel,
        out_shape=(
            pltpu.VMEM((TILES * 128, C), BF16),
            pltpu.VMEM((2, TILES), F32),
        ),
        in_specs=[hbm] * 8,
        out_specs=(vmem, vmem),
        scratch_shapes=[
            pltpu.VMEM((TILES, 128), jnp.int32),
            pltpu.VMEM((2, N), jnp.int32),
            pltpu.VMEM((2, N), jnp.int32),
            pltpu.VMEM((1, N), jnp.int32),
            pltpu.VMEM((1, 2304), jnp.int32),
            pltpu.VMEM((TILES * 16, 8, C), BF16),
            pltpu.VMEM((TILES * 16, 8, C), BF16),
            pltpu.VMEM((4, 16, 8, C), BF16),
            pltpu.VMEM((TILES, 3, 128, 128), BF16),
            pltpu.VMEM((N, 2, 8, 128), BF16),
            pltpu.VMEM((2048, 128), BF16),
            pltpu.VMEM((128, 2048), BF16),
            pltpu.VMEM((1, 2304), jnp.int32),
            pltpu.VMEM((TILES * 128, C), F32),
            pltpu.VMEM((TILES * 128, 128), F32),
            pltpu.VMEM((TILES * 128, 128), F32),
            pltpu.VMEM((N, 1, N), jnp.int32),
            pltpu.VMEM((N, 1, N), jnp.int32),
            pltpu.VMEM((N, N), jnp.int32),
            pltpu.SMEM((8, N), jnp.int32),
            pltpu.VMEM((2 * N, 8, C), BF16),
            pltpu.VMEM((2 * N, 8, C), BF16),
            pltpu.VMEM((2 * N, 8, C), BF16),
            pltpu.VMEM((2 * TILES, 8, 128), F32),
            pltpu.VMEM((TILES, 128), F32),
            dma((8,)), dma, dma, dma, dma((2,)), dma((16,)), dma((4,)), dma((4,)),
        ],
        compiler_params=pltpu.CompilerParams(
            collective_id=0, has_side_effects=True, vmem_limit_bytes=48 << 20
        ),
    )(*[
        pltpu.with_memory_space_constraint(x, pltpu.HBM)
        for x in (
            labels.reshape(TILES * 16, 8, C),
            seed_mask.reshape(TILES, 128),
            band_w,
            jnp.swapaxes(far_block, 1, 2)[0],
            jnp.swapaxes(far_tile, 1, 2)[0],
            far_count,
            far_w[0],
            jnp.asarray(np.concatenate([np.repeat(code, 16), np.repeat(code, 2)])[None]),
        )
    ])
    return out, res


def solution(mesh):
    placed = (
        P("node", None),
        P("node"),
        P("node", None, None, None),
        P("node", None, None),
        P("node", None, None),
        P("node", None),
        P("node", None, None, None, None),
    )
    return jax.shard_map(
        body,
        mesh=mesh,
        in_specs=placed,
        out_specs=(P("node", None), P(None, "node")),
        check_vma=False,
    )
```
